32 devices in a mesh: wide: 4 (over x, core), narrow: 8 (over z, y).
Axes of the slice: x: 2, y: 2, z: 4, core: 2. Of those that a mesh axis runs over, the one named last changes fastest.
Arguments:
- single: bfloat16 [48, 128, 768], P('narrow', 'wide'), may hold values from -6 to 6
- pair: bfloat16 [128, 128, 128], P('wide', 'narrow'), may hold values from -6 to 6
- restype: int32 [128], P('wide'), may hold values from 0 to 31
- chain: int32 [128], replicated, may hold values from 0 to 7, never falling along the last dimension, each value on 1 to 32 neighbouring positions
- residue_type_embedding: float32 [32, 768], replicated, may hold values from -6 to 6
- pair_bias_weight: bfloat16 [2, 16, 128], replicated, may hold values from -41 to 41, as said below
- shared_chain_score: float32 [2, 16], replicated, may hold values from -8 to 8
- query_weight: bfloat16 [2, 768, 768], replicated, may hold values from -0.21875 to 0.21875
- key_weight: bfloat16 [2, 768, 768], replicated, may hold values from -0.21875 to 0.21875
- value_weight: bfloat16 [2, 768, 768], replicated, may hold values from -0.21875 to 0.21875
- output_weight: bfloat16 [2, 768, 768], replicated, may hold values from -0.21875 to 0.21875
Outputs:
- updated: bfloat16 [48, 128, 768], P('narrow', 'wide')
The draws below stay inside these ranges and needn't reach their ends.
Inputs may be any that keep to these rules, and one draw needn't show every extreme that they name: `pair_bias_weight`: each entry is a real number.
All inputs are finite; a program needn't handle non-finite values.
Results may differ from the reference program's by a relative error of at most 0.0084.
Values may be sent and summed in bfloat16 or wider, within the bound.
No kernel may reach another device: no remote copies, remote signals or barrier semaphores. Data moves between devices by JAX's collectives and lax.ppermute only.
A program may use at most 128 MiB of HBM per device.

```python
import math
import jax
import jax.numpy as jnp
import numpy as np
from jax import lax

D = 768
HEAD_TOTAL = 16
HEAD_DIM = 48
PAIR_C = 128
TYPES = 32
CHAINS = 8
BLOCK_TOTAL = 2
SAMPLES = 48
TOKENS = 128


def draw_pair_bias_weight(key, part):
    base_key = jax.random.fold_in(jax.random.fold_in(key, 17), 0)
    values = 0.27 * jax.random.truncated_normal(base_key, -6.0, 6.0, (BLOCK_TOTAL, HEAD_TOTAL, PAIR_C), jnp.float32)
    return values.astype(jnp.bfloat16)


def touch_ends(result, stream_key, least, largest):
    extent = result.shape
    place = [jax.random.randint(jax.random.fold_in(stream_key, axis), (), 0, extent[axis]) for axis in range(len(extent))]
    result = result.at[tuple(place)].set(least)
    longest = extent.index(max(extent))
    place[longest] = (place[longest] + 1) % extent[longest]
    return result.at[tuple(place)].set(largest)


def block_levels(key, shape, shards, smallest, high):
    factor_of = 1.0
    for dim, blocks in shards:
        steps = jax.random.uniform(jax.random.fold_in(jax.random.fold_in(key, 6), dim), (blocks,), jnp.float32, smallest / len(shards), high / len(shards))
        factor_of = factor_of * jnp.repeat(jnp.exp(steps), shape[dim] // blocks).reshape((-1,) + (1,) * (len(shape) - 1 - dim))
    return factor_of


def split_up(count, total, most, lean):
    weights = [(1 << 20) // math.isqrt(standing ** lean) + 1 for standing in range(2, count + 1)]
    spare, counts = total - most - (count - 1), [1] * (count - 1)
    while spare > 0:
        movable = [i for i in range(count - 1) if counts[i] < most]
        whole, remaining = sum([weights[i] for i in movable]), spare
        for i in movable:
            extra = min(most - counts[i], max(1, remaining * weights[i] // whole), spare)
            counts[i] = counts[i] + extra
            spare = spare - extra
    return np.array([most] + counts)


def uneven(rng, count, total, most, lean):
    if count == 2:
        one = jax.random.randint(rng, (), max(1, total - most), min(most, total - 1) + 1)
        return jnp.stack([one, total - one])
    tallies = jnp.asarray(split_up(count, total, most, lean), jnp.int32)
    twos = (count - 1) // 2
    donor, taker = tallies[1:1 + 2 * twos:2], tallies[2:2 + 2 * twos:2]
    margin = jnp.minimum(donor - 1, most - taker)
    shifted = jax.random.randint(jax.random.fold_in(rng, 1), (twos,), 0, 1 << 20) % (margin + 1)
    tallies = tallies.at[1:1 + 2 * twos:2].set(donor - shifted).at[2:2 + 2 * twos:2].set(taker + shifted)
    return tallies[jax.random.permutation(jax.random.fold_in(rng, 2), count)]


def bell_draw(stream_key, extent, spread, reach, pieces=(), held_as=jnp.bfloat16):
    level = block_levels(stream_key, extent, pieces, -0.22, 0.18) if pieces else 1.0
    values = jax.random.normal(stream_key, extent, jnp.float32) * spread * level
    return jnp.minimum(jnp.maximum(values, -reach), reach).astype(held_as)


def setup_inputs(seed: int = 0) -> dict:
    key_list = jax.random.split(jax.random.key(seed), 12)
    single = bell_draw(key_list[0], (SAMPLES, TOKENS, D), 1.0, 6.0, ((0, 8), (1, 4)))
    pair = bell_draw(key_list[1], (TOKENS, TOKENS, PAIR_C), 1.0, 6.0, ((0, 4), (1, 8)))
    restype = touch_ends(jax.random.randint(key_list[2], (TOKENS,), 0, TYPES), jax.random.fold_in(key_list[2], 1), 0, TYPES - 1).astype(jnp.int32)
    chain = jnp.searchsorted(jnp.cumsum(uneven(key_list[3], CHAINS, TOKENS, TOKENS // 4, 1)), jnp.arange(TOKENS), side="right").astype(jnp.int32)
    residue_type_embedding = bell_draw(key_list[4], (TYPES, D), 1.0, 6.0, (), jnp.float32)
    pair_bias_weight = draw_pair_bias_weight(jax.random.fold_in(key_list[11], 71), 0)
    shared_chain_score = bell_draw(key_list[6], (BLOCK_TOTAL, HEAD_TOTAL), 2.0, 8.0, (), jnp.float32)
    query_weight = bell_draw(key_list[7], (BLOCK_TOTAL, D, D), D ** -0.5, 0.21875)
    key_weight = bell_draw(key_list[8], (BLOCK_TOTAL, D, D), D ** -0.5, 0.21875)
    value_weight = bell_draw(key_list[9], (BLOCK_TOTAL, D, D), D ** -0.5, 0.21875)
    output_weight = bell_draw(key_list[10], (BLOCK_TOTAL, D, D), D ** -0.5, 0.21875)
    return {"single": single, "pair": pair, "restype": restype, "chain": chain, "residue_type_embedding": residue_type_embedding, "pair_bias_weight": pair_bias_weight, "shared_chain_score": shared_chain_score, "query_weight": query_weight, "key_weight": key_weight, "value_weight": value_weight, "output_weight": output_weight}


epsilon_norm = 1e-05

def normalize(inputs):
    average = lax.optimization_barrier(jnp.mean(inputs, axis=-1, keepdims=True))
    centered = inputs - average
    spread_squared = lax.optimization_barrier(jnp.mean(centered * centered, axis=-1, keepdims=True))
    return centered * lax.rsqrt(spread_squared + epsilon_norm)

def reference(single, pair, restype, chain, residue_type_embedding, pair_bias_weight, shared_chain_score, query_weight, key_weight, value_weight, output_weight):
    onehot = (restype[:, None] == jnp.arange(TYPES, dtype=jnp.int32)[None, :]).astype(jnp.float32)
    embedded = jnp.dot(onehot, residue_type_embedding, precision=lax.Precision.HIGHEST)
    residual = single.astype(jnp.float32) + embedded[None]
    pair_norm = normalize(pair.astype(jnp.float32)).astype(jnp.bfloat16)
    same_strand_indicator = (chain[:, None] == chain[None, :]).astype(jnp.float32)
    score_scale = 1.0 / math.sqrt(HEAD_DIM)
    for present_segment_index in range(BLOCK_TOTAL):
        layer_head_bias = jnp.einsum('ijc,hc->hij', pair_norm.astype(jnp.float32), pair_bias_weight[present_segment_index].astype(jnp.float32))
        layer_head_bias = layer_head_bias + shared_chain_score[present_segment_index][:, None, None] * same_strand_indicator[None]
        normed = normalize(residual).astype(jnp.bfloat16)
        reshaped_flat_array = normed.reshape(SAMPLES * TOKENS, D)
        queries = jnp.dot(reshaped_flat_array, query_weight[present_segment_index], preferred_element_type=jnp.float32).astype(jnp.bfloat16).reshape(SAMPLES, TOKENS, HEAD_TOTAL, HEAD_DIM)
        key_rows = jnp.dot(reshaped_flat_array, key_weight[present_segment_index], preferred_element_type=jnp.float32).astype(jnp.bfloat16).reshape(SAMPLES, TOKENS, HEAD_TOTAL, HEAD_DIM)
        value_rows = jnp.dot(reshaped_flat_array, value_weight[present_segment_index], preferred_element_type=jnp.float32).astype(jnp.bfloat16).reshape(SAMPLES, TOKENS, HEAD_TOTAL, HEAD_DIM)

        def attend(operands):
            query_one, key_one, value_one = operands
            scores = jnp.einsum('qhd,khd->hqk', query_one.astype(jnp.float32), key_one.astype(jnp.float32)) * score_scale + layer_head_bias
            largest_logit = lax.optimization_barrier(jnp.max(scores, axis=-1, keepdims=True))
            weights_exp = jnp.exp(scores - largest_logit)
            summed = lax.optimization_barrier(jnp.sum(weights_exp, axis=-1))
            probs = weights_exp.astype(jnp.bfloat16)
            mixed = jnp.einsum('hqk,khd->qhd', probs.astype(jnp.float32), value_one.astype(jnp.float32))
            return (mixed / jnp.transpose(summed)[:, :, None]).astype(jnp.bfloat16)
        attended = lax.map(attend, (queries, key_rows, value_rows))
        projected = jnp.dot(attended.reshape(SAMPLES * TOKENS, D), output_weight[present_segment_index], preferred_element_type=jnp.float32)
        residual = residual + projected.reshape(SAMPLES, TOKENS, D)
    return residual.astype(jnp.bfloat16)
```

```python
import functools
import math

import jax
import jax.numpy as jnp
from jax import lax
from jax.experimental import pallas as pl
from jax.experimental.pallas import tpu as pltpu
from jax.sharding import PartitionSpec as P

epsilon_norm = 1e-05
LANES = 128
WINDOW = 256


def normalize(inputs):
    average = jnp.mean(inputs, axis=-1, keepdims=True)
    centered = inputs - average
    spread_squared = jnp.mean(centered * centered, axis=-1, keepdims=True)
    return centered * lax.rsqrt(spread_squared + epsilon_norm)


def attend(stacked, layer_head_bias, score_scale):
    head_dim = stacked.shape[-1] // 3
    queries = stacked[..., :head_dim]
    key_rows = stacked[..., head_dim : 2 * head_dim]
    value_rows = stacked[..., 2 * head_dim :]
    key_piece = lax.all_gather(key_rows, "wide", axis=1, tiled=True)
    value_piece = lax.all_gather(value_rows, "wide", axis=1, tiled=True)
    scores = (
        jnp.einsum("aqhd,akhd->ahqk", queries, key_piece, preferred_element_type=jnp.float32)
        * score_scale
        + layer_head_bias[None]
    )
    weights_exp = jnp.exp(scores - jnp.max(scores, axis=-1)[..., None])
    total = jnp.sum(weights_exp, axis=-1)
    mixed = jnp.einsum(
        "ahqk,akhd->aqhd",
        weights_exp.astype(jnp.bfloat16),
        value_piece,
        preferred_element_type=jnp.float32,
    )
    return (mixed / jnp.swapaxes(total, 1, 2)[..., None]).astype(jnp.bfloat16)


def general_shards(
    single,
    pair,
    restype,
    chain,
    residue_type_embedding,
    pair_bias_weight,
    shared_chain_score,
    query_weight,
    key_weight,
    value_weight,
    output_weight,
):
    sample_count, row_count, model_width = single.shape
    head_count = pair_bias_weight.shape[1]
    head_dim = model_width // head_count
    block_count = query_weight.shape[0]
    row_begin = lax.axis_index("wide") * row_count
    onehot = (
        restype[:, None] == jnp.arange(residue_type_embedding.shape[0], dtype=jnp.int32)[None, :]
    ).astype(jnp.float32)
    embedded = jnp.dot(onehot, residue_type_embedding, precision=lax.Precision.HIGHEST)
    residual = single.astype(jnp.float32) + embedded[None]
    pair_norm = normalize(pair.astype(jnp.float32)).astype(jnp.bfloat16)
    bias_panel = jnp.einsum(
        "ijc,bhc->hbij", pair_norm, pair_bias_weight, preferred_element_type=jnp.float32
    )
    row_chain = lax.dynamic_slice_in_dim(chain, row_begin, row_count)
    same_strand_indicator = (row_chain[:, None] == chain[None, :]).astype(jnp.float32)
    complete_bias = lax.all_gather(bias_panel, "narrow", axis=3, tiled=True)
    score_scale = 1.0 / math.sqrt(head_dim)
    for block in range(block_count):
        layer_head_bias = (
            complete_bias[:, block]
            + shared_chain_score[block][:, None, None] * same_strand_indicator[None]
        )
        normed = normalize(residual).astype(jnp.bfloat16).reshape(-1, model_width)
        parts = [
            jnp.dot(normed, weight[block], preferred_element_type=jnp.float32)
            .astype(jnp.bfloat16)
            .reshape(sample_count, row_count, head_count, head_dim)
            for weight in (query_weight, key_weight, value_weight)
        ]
        regrouped = attend(jnp.concatenate(parts, axis=-1), layer_head_bias, score_scale)
        projected = jnp.dot(
            regrouped.reshape(-1, model_width),
            output_weight[block],
            preferred_element_type=jnp.float32,
        )
        residual = residual + projected.reshape(residual.shape)
    return residual.astype(jnp.bfloat16)


def layer_norm_kernel(restype, single, embedding, residual, normed, embedded):
    for row in range(embedded.shape[0]):
        embedded[pl.ds(row, 1), :] = embedding[pl.ds(restype[row], 1), :]
    total = single[...].astype(jnp.float32) + embedded[...][None]
    residual[...] = total
    normed[...] = normalize(total).astype(jnp.bfloat16)


def bias_kernel(pair, weight, shared, *outs):
    rows, columns, channels = pair.shape
    blocks, heads, _ = weight.shape
    group = LANES // heads
    normed = normalize(pair[...].astype(jnp.float32)).astype(jnp.bfloat16)
    normed = normed.reshape(rows // group, group, columns, channels)
    for block in range(blocks):
        total = shared[block]
        for step in range(group):
            pieces = [jnp.zeros((heads, channels), jnp.bfloat16)] * group
            pieces[step] = weight[block]
            spread = jnp.concatenate(pieces, axis=0)
            part = normed[:, step].reshape(rows // group * columns, channels)
            total = total + lax.dot_general(
                part, spread, (((1,), (1,)), ((), ())), preferred_element_type=jnp.float32
            )
        outs[block][...] = total


def head_groups(heads, head_dim):
    groups = []
    for head in range(heads):
        offset = head * head_dim // LANES * LANES
        if groups and (head + 1) * head_dim <= groups[-1][0] + WINDOW:
            groups[-1][1].append(head)
        else:
            groups.append((min(offset, heads * head_dim - WINDOW), [head]))
    return groups


def block_kernel(block, last, slots, *refs):
    chunks = refs[:4]
    near, far, residual, wq, wk, wv, wo = refs[4:11]
    if last:
        outs, scratch = refs[11:12], refs[12:]
    else:
        outs, scratch = refs[11:13], refs[13:]
    weights, keys, values, queries, attended, turned, bias, sems = scratch
    samples, rows, width = residual.shape
    tokens = keys.shape[1]
    heads = bias.shape[0] // rows
    head_dim = width // heads
    scale = 1.0 / math.sqrt(head_dim)
    order = (1, 2, 0, 3)
    sources = (wq, wk, wv, wo)
    copies = {}
    for which in order:
        copies[which] = pltpu.make_async_copy(
            sources[which].at[block], weights.at[which], sems.at[which]
        )
        copies[which].start()

    shard = near.shape[1] // turned.shape[0]
    for side, ref in enumerate((near, far)):
        for step in range(ref.shape[0]):
            place = pl.multiple_of(slots[4 + side * 4 + step] * shard, shard)
            for piece in range(turned.shape[0]):
                turned[piece, pl.ds(place, shard), :] = ref[
                    step, piece * shard : (piece + 1) * shard, :
                ]
    for piece in range(turned.shape[0]):
        bias[piece * LANES : (piece + 1) * LANES, :] = turned[piece].T

    def project(ref, which):
        flat = ref[...].reshape(samples * rows, width)
        out = jnp.dot(flat, weights[which], preferred_element_type=jnp.float32)
        return out.astype(jnp.bfloat16).reshape(samples, rows, width)

    for which, dest in ((1, keys), (2, values)):
        copies[which].wait()
        for step in range(4):
            place = pl.multiple_of(slots[step] * rows, rows)
            dest[:, pl.ds(place, rows), :] = project(chunks[step], which)
    copies[0].wait()
    queries[...] = project(chunks[0], 0)

    groups = head_groups(heads, head_dim)

    def sample_step(sample, carry):
        tiles = [None] * (width // LANES)
        lane = lax.broadcasted_iota(jnp.int32, (rows, WINDOW), 1)
        for offset, members in groups:
            window = queries[sample, :, offset : offset + WINDOW]
            masked = []
            for head in members:
                low = head * head_dim - offset
                inside = (lane >= low) & (lane < low + head_dim)
                masked.append(jnp.where(inside, window, jnp.zeros_like(window)))
            stacked = jnp.concatenate(masked, axis=0)
            scores = lax.dot_general(
                stacked,
                keys[sample, :, offset : offset + WINDOW],
                (((1,), (1,)), ((), ())),
                preferred_element_type=jnp.float32,
            )
            added = jnp.concatenate(
                [bias[pl.ds(head, rows, stride=heads), :] for head in members], axis=0
            )
            scores = scores * scale + added
            peak = jnp.max(scores, axis=-1, keepdims=True)
            expo = jnp.exp(scores - peak)
            total = jnp.sum(expo, axis=-1, keepdims=True)
            mixed = jnp.dot(
                expo.astype(jnp.bfloat16),
                values[sample, :, offset : offset + WINDOW],
                preferred_element_type=jnp.float32,
            )
            inverse = 1.0 / total
            for place, head in enumerate(members):
                first, after = head * head_dim, (head + 1) * head_dim
                span = slice(place * rows, (place + 1) * rows)
                for tile in range(first // LANES, (after - 1) // LANES + 1):
                    begin = tile * LANES - offset
                    share = mixed[span, begin : begin + LANES] * inverse[span]
                    position = tile * LANES + lane[:, :LANES]
                    if tiles[tile] is None:
                        tiles[tile] = share
                    else:
                        tiles[tile] = jnp.where(position >= first, share, tiles[tile])
        attended[sample] = jnp.concatenate(tiles, axis=1).astype(jnp.bfloat16)
        return carry

    lax.fori_loop(0, samples, sample_step, 0)
    copies[3].wait()
    flat = attended[...].reshape(samples * rows, width)
    projected = jnp.dot(flat, weights[3], preferred_element_type=jnp.float32)
    fresh = residual[...] + projected.reshape(samples, rows, width)
    if last:
        outs[0][...] = fresh.astype(jnp.bfloat16)
    else:
        outs[0][...] = fresh
        outs[1][...] = normalize(fresh).astype(jnp.bfloat16)


def vmem():
    return pl.BlockSpec(memory_space=pltpu.VMEM)


def fused_shards(
    wide,
    narrow,
    single,
    pair,
    restype,
    chain,
    residue_type_embedding,
    pair_bias_weight,
    shared_chain_score,
    query_weight,
    key_weight,
    value_weight,
    output_weight,
):
    samples, rows, width = single.shape
    columns = pair.shape[1]
    blocks, heads, channels = pair_bias_weight.shape
    group = LANES // heads
    across = lax.axis_index("wide")
    along = lax.axis_index("narrow")
    smem = pl.BlockSpec(memory_space=pltpu.SMEM)
    limit = 40 << 20

    residual, normed = pl.pallas_call(
        layer_norm_kernel,
        out_shape=(
            jax.ShapeDtypeStruct(single.shape, jnp.float32),
            jax.ShapeDtypeStruct(single.shape, jnp.bfloat16),
        ),
        in_specs=[smem, vmem(), vmem()],
        out_specs=(vmem(), vmem()),
        scratch_shapes=[pltpu.VMEM((rows, width), jnp.float32)],
        name="layer_norm",
    )(restype, single, residue_type_embedding)

    row_chain = lax.dynamic_slice_in_dim(chain, across * rows, rows)
    column_chain = lax.dynamic_slice_in_dim(chain, along * columns, columns)
    same = row_chain.reshape(-1, 1, group, 1) == column_chain[None, :, None, None]
    shared = jnp.where(same[None], shared_chain_score[:, None, None, None, :], 0.0)
    panel_shape = (rows // group * columns, LANES)
    shared = shared.reshape(blocks, *panel_shape)
    panels = pl.pallas_call(
        bias_kernel,
        out_shape=tuple(jax.ShapeDtypeStruct(panel_shape, jnp.float32) for _ in range(blocks)),
        in_specs=[vmem()] * 3,
        out_specs=tuple(vmem() for _ in range(blocks)),
        name="pair_bias",
    )(pair, pair_bias_weight, shared)

    def swap(value, axis, mask):
        size = wide if axis == "wide" else narrow
        return lax.ppermute(value, axis, [(i, i ^ mask) for i in range(size)])

    slots = jnp.stack(
        [across ^ mask for mask in range(wide)]
        + [along ^ mask for mask in range(0, narrow, 2)]
        + [along ^ mask for mask in range(1, narrow, 2)]
    ).astype(jnp.int32)

    sides = []
    for panel in panels:
        near = jnp.stack([panel] + [swap(panel, "narrow", mask) for mask in range(2, narrow, 2)])
        sides.append((near, swap(near, "narrow", 1)))

    for block in range(blocks):
        last = block == blocks - 1
        beside = swap(normed, "wide", 1)
        opposite = swap(normed, "wide", 2)
        chunks = (normed, beside, opposite, swap(opposite, "wide", 1))
        tokens = wide * rows
        if last:
            out_shape = (jax.ShapeDtypeStruct(single.shape, jnp.bfloat16),)
        else:
            out_shape = (
                jax.ShapeDtypeStruct(single.shape, jnp.float32),
                jax.ShapeDtypeStruct(single.shape, jnp.bfloat16),
            )
        outs = pl.pallas_call(
            functools.partial(block_kernel, block, last),
            out_shape=out_shape,
            in_specs=[smem] + [vmem()] * 7 + [pl.BlockSpec(memory_space=pl.ANY)] * 4,
            out_specs=tuple(vmem() for _ in out_shape),
            scratch_shapes=[
                pltpu.VMEM((4, width, width), jnp.bfloat16),
                pltpu.VMEM((samples, tokens, width), jnp.bfloat16),
                pltpu.VMEM((samples, tokens, width), jnp.bfloat16),
                pltpu.VMEM((samples, rows, width), jnp.bfloat16),
                pltpu.VMEM((samples, rows, width), jnp.bfloat16),
                pltpu.VMEM((rows // group, tokens, LANES), jnp.float32),
                pltpu.VMEM((rows * heads, tokens), jnp.float32),
                pltpu.SemaphoreType.DMA((4,)),
            ],
            compiler_params=pltpu.CompilerParams(vmem_limit_bytes=limit),
            cost_estimate=pl.CostEstimate(
                flops=2 * samples * rows * width * width * 10,
                bytes_accessed=4 * width * width * 2,
                transcendentals=samples * rows * heads * tokens,
            ),
            name="block",
        )(
            slots,
            *chunks,
            *sides[block],
            residual,
            query_weight,
            key_weight,
            value_weight,
            output_weight,
        )
        if last:
            return outs[0]
        residual, normed = outs


def fits_fused(mesh, single, pair, pair_bias_weight):
    wide, narrow = mesh.shape["wide"], mesh.shape["narrow"]
    _, heads, channels = pair_bias_weight.shape
    width = single.shape[-1]
    rows, columns = pair.shape[0] // wide, pair.shape[1] // narrow
    head_dim = width // heads
    return (
        wide == 4
        and narrow == 8
        and pair.shape[1] == LANES
        and channels == LANES
        and LANES % heads == 0
        and rows % max(LANES // heads, 16) == 0
        and columns % 16 == 0
        and width % LANES == 0
        and width >= WINDOW
        and head_dim <= LANES
    )


def solution(mesh):
    def run(*args):
        single, pair, pair_bias_weight = args[0], args[1], args[5]
        if fits_fused(mesh, single, pair, pair_bias_weight):
            body = functools.partial(fused_shards, mesh.shape["wide"], mesh.shape["narrow"])
        else:
            body = general_shards
        return jax.shard_map(
            body,
            mesh=mesh,
            in_specs=(
                P("narrow", "wide", None),
                P("wide", "narrow", None),
                P("wide"),
                P(),
                P(),
                P(),
                P(),
                P(),
                P(),
                P(),
                P(),
            ),
            out_specs=P("narrow", "wide", None),
            check_vma=False,
        )(*args)

    return run
```
